8 devices in a mesh: depth: 2 (over z, y), col: 2 (over x), row: 2 (over core).
Axes of the slice: x: 2, y: 2, z: 1, core: 2. Of those that a mesh axis runs over, the one named last changes fastest.
Arguments:
- a_mat: bfloat16 [12288, 12288], P('row', 'col')
- b_mat: bfloat16 [12288, 12288], P('row', 'col')
Outputs:
- output: bfloat16 [12288, 12288], P(('row', 'depth'), 'col')
All inputs are finite; a program needn't handle non-finite values.
Results may differ from the reference program's by a relative error of at most 0.001.
Values are sent between devices in bfloat16 or wider.
A program may use at most 1 GiB of HBM per device.

```python
import jax
import jax.numpy as jnp

D = 12288


def setup_inputs(seed: int = 0) -> dict:
    key_a, key_b = jax.random.split(jax.random.key(seed))
    a_mat = jax.random.normal(key_a, (D, D), jnp.float32) + 0.5
    b_mat = (jax.random.normal(key_b, (D, D), jnp.float32) + 2.0 * D ** -0.5) * D ** -0.5
    return {"a_mat": a_mat.astype(jnp.bfloat16), "b_mat": b_mat.astype(jnp.bfloat16)}


def reference(a_mat, b_mat):
    return jnp.dot(a_mat, b_mat, preferred_element_type=jnp.float32).astype(jnp.bfloat16)
```

```python
import functools

import jax
import jax.numpy as jnp
from jax import lax
from jax.experimental import pallas as pl
from jax.experimental.pallas import tpu as pltpu
from jax.sharding import PartitionSpec as P

PIECES = (
    (2560, 128, (0, 6144)),
    (0, 512, (0, 6144)),
    (512, 512, (0, 6144)),
    (1024, 512, (0, 6144)),
    (1536, 512, (0, 6144)),
    (2048, 512, (0, 6144)),
    (2688, 384, (0, 2048, 4096, 5120, 5632, 6144)),
)


def mm_kernel(n_blk, depth, k_off, k_len, own, with_part, meta_ref, a_ref, b_loc, b_rcv, *refs):
    if with_part:
        part_ref, refs = refs[0], refs[1:]
    out_ref, b_buf, sems = refs[-3], refs[-2], refs[-1]
    row_blk, col_blk = pl.program_id(0), pl.program_id(1)
    n_steps = pl.num_programs(0) * pl.num_programs(1)
    step = row_blk * pl.num_programs(1) + col_blk
    take_loc = meta_ref[1] == (1 if own else 0)

    def fetch(blk, slot):
        cols = pl.ds(pl.multiple_of(blk * n_blk, n_blk), n_blk)

        @pl.when(take_loc)
        def _():
            pltpu.make_async_copy(b_loc.at[pl.ds(k_off, k_len), cols], b_buf.at[slot], sems.at[slot]).start()

        @pl.when(jnp.logical_not(take_loc))
        def _():
            pltpu.make_async_copy(b_rcv.at[pl.ds(k_off, k_len), cols], b_buf.at[slot], sems.at[slot]).start()

    slot = lax.rem(step, depth)

    @pl.when(step == 0)
    def _():
        for ahead in range(depth - 1):
            fetch(ahead, ahead)

    @pl.when(step + depth - 1 < n_steps)
    def _():
        fetch(lax.rem(step + depth - 1, pl.num_programs(1)), lax.rem(step + depth - 1, depth))

    pltpu.make_async_copy(b_loc.at[pl.ds(k_off, k_len), pl.ds(0, n_blk)], b_buf.at[slot], sems.at[slot]).wait()
    prod = jnp.dot(a_ref[...], b_buf[slot], preferred_element_type=jnp.float32)
    if with_part:
        prod = part_ref[...] + prod
    out_ref[...] = prod.astype(out_ref.dtype)


def mm_call(meta, a_arr, b_loc, b_rcv, part, out_buf, *, m_blk, n_rows, a_by_layer, k_off, k_len, row_off, part_off, out_off,
            out_shape, own, name):
    n_side = b_loc.shape[1]
    n_blk = 512 if k_len > 4096 else 1024 if k_len > 1024 else 2048
    depth = 2 if m_blk > 512 else 3
    grid = (n_rows // m_blk, n_side // n_blk)
    a_step = (b_loc.shape[0] // 2) // m_blk

    def a_map(r, c, meta_ref):
        return (meta_ref[0] * a_step + r if a_by_layer else r, 0)

    in_specs = [pl.BlockSpec((m_blk, k_len), a_map), pl.BlockSpec(memory_space=pl.ANY), pl.BlockSpec(memory_space=pl.ANY)]
    operands = [a_arr, b_loc, b_rcv]
    if part is not None:
        in_specs.append(pl.BlockSpec((m_blk, n_blk), lambda r, c, meta_ref: (part_off // m_blk + r, c)))
        operands.append(part)
    aliases = {}
    if out_buf is not None:
        in_specs.append(pl.BlockSpec(memory_space=pl.ANY))
        operands.append(out_buf)
        aliases = {len(operands): 0}
    return pl.pallas_call(
        functools.partial(mm_kernel, n_blk, depth, k_off, k_len, own, part is not None),
        out_shape=out_shape,
        grid_spec=pltpu.PrefetchScalarGridSpec(
            num_scalar_prefetch=1,
            grid=grid,
            in_specs=in_specs,
            out_specs=pl.BlockSpec((m_blk, n_blk), lambda r, c, meta_ref: (out_off // m_blk + r, c)),
            scratch_shapes=[pltpu.VMEM((depth, k_len, n_blk), jnp.bfloat16), pltpu.SemaphoreType.DMA((depth,))],
        ),
        input_output_aliases=aliases,
        cost_estimate=pl.CostEstimate(
            flops=2 * n_rows * k_len * n_side, bytes_accessed=2 * (n_rows + n_side) * k_len + 6 * n_rows * n_side, transcendentals=0
        ),
        compiler_params=pltpu.CompilerParams(
            dimension_semantics=("arbitrary", "arbitrary"), vmem_limit_bytes=60 * 1024 * 1024
        ),
        name=name,
    )(meta, *operands)


def solution(mesh):
    swap = [(0, 1), (1, 0)]

    def local_mm(a_blk, b_blk):
        side = a_blk.shape[0]
        half = side // 2
        layer_idx = lax.axis_index("depth")
        row_idx = lax.axis_index("row")
        col_idx = lax.axis_index("col")
        meta = jnp.stack([layer_idx, (row_idx == col_idx).astype(jnp.int32)]).astype(jnp.int32)

        pieces = []
        for row0, rows, cuts in PIECES:
            for k0, k1 in zip(cuts[:-1], cuts[1:]):
                pieces.append((row0, rows, k0, k1))
        moved = []
        for row0, rows, k0, k1 in pieces:
            part_a = lax.dynamic_slice(a_blk, (layer_idx * half + row0, k0), (rows, k1 - k0))
            moved.append(lax.ppermute(part_a, "col", swap))
            if len(moved) == 1:
                b_rcv = lax.ppermute(b_blk, "row", swap)

        call = functools.partial(mm_call, meta, b_loc=b_blk, b_rcv=b_rcv)
        part = call(
            a_blk, part=None, out_buf=None, m_blk=1024, n_rows=half, a_by_layer=True, k_off=0, k_len=side, row_off=0, part_off=0,
            out_off=0, out_shape=jax.ShapeDtypeStruct((half, side), jnp.float32), own=True, name="own_part",
        )
        out = None
        partial_sums = {}
        for (row0, rows, k0, k1), a_piece in zip(pieces, moved):
            first, last = k0 == 0, k1 == side
            src, src_off = (part, row0) if first else (partial_sums[row0], 0)
            if last:
                shape = jax.ShapeDtypeStruct((half, side), jnp.bfloat16)
            else:
                shape = jax.ShapeDtypeStruct((rows, side), jnp.float32)
            res = call(
                a_piece, part=src, out_buf=out if last else None, m_blk=rows, n_rows=rows, a_by_layer=False, k_off=k0,
                k_len=k1 - k0, row_off=0, part_off=src_off, out_off=row0 if last else 0, out_shape=shape, own=False,
                name=f"piece_{row0}_{k0}",
            )
            if last:
                out = res
            else:
                partial_sums[row0] = res
        return out

    spec_in = P("row", "col")
    spec_out = P(("row", "depth"), "col")
    return jax.shard_map(local_mm, mesh=mesh, in_specs=(spec_in, spec_in), out_specs=spec_out, check_vma=False)
```

```python
import functools

import jax
import jax.numpy as jnp
from jax import lax
from jax.experimental import pallas as pl
from jax.experimental.pallas import tpu as pltpu
from jax.sharding import PartitionSpec as P

PIECES = ((2560, 128), (0, 512), (512, 512), (1024, 512), (1536, 512), (2048, 512))
LAST_ROWS = (2688, 384)
LAST_BOXES = ((0, 384, 0, 2048), (0, 384, 2048, 4096), (0, 384, 4096, 5120), (0, 256, 5120, 6144), (256, 128, 5120, 6144))
HELD_FROM = 5120


def mm_kernel(n_blk, depth, k_off, k_len, own, with_part, meta_ref, a_ref, b_loc, b_rcv, *refs):
    if with_part:
        part_ref, refs = refs[0], refs[1:]
    out_ref, b_buf, sems = refs[-3], refs[-2], refs[-1]
    row_blk, col_blk = pl.program_id(0), pl.program_id(1)
    n_steps = pl.num_programs(0) * pl.num_programs(1)
    step = row_blk * pl.num_programs(1) + col_blk
    take_loc = meta_ref[1] == (1 if own else 0)

    def fetch(blk, slot):
        cols = pl.ds(pl.multiple_of(blk * n_blk, n_blk), n_blk)

        @pl.when(take_loc)
        def _():
            pltpu.make_async_copy(b_loc.at[pl.ds(k_off, k_len), cols], b_buf.at[slot], sems.at[slot]).start()

        @pl.when(jnp.logical_not(take_loc))
        def _():
            pltpu.make_async_copy(b_rcv.at[pl.ds(k_off, k_len), cols], b_buf.at[slot], sems.at[slot]).start()

    slot = lax.rem(step, depth)

    @pl.when(step == 0)
    def _():
        for ahead in range(depth - 1):
            fetch(ahead, ahead)

    @pl.when(step + depth - 1 < n_steps)
    def _():
        fetch(lax.rem(step + depth - 1, pl.num_programs(1)), lax.rem(step + depth - 1, depth))

    pltpu.make_async_copy(b_loc.at[pl.ds(k_off, k_len), pl.ds(0, n_blk)], b_buf.at[slot], sems.at[slot]).wait()
    prod = jnp.dot(a_ref[...], b_buf[slot], preferred_element_type=jnp.float32)
    if with_part:
        prod = part_ref[...] + prod
    out_ref[...] = prod.astype(out_ref.dtype)


def mm_call(meta, a_arr, b_loc, b_rcv, part, out_buf, *, m_blk, n_rows, a_by_layer, k_off, k_len, row_off, part_off, out_off,
            out_shape, own, name):
    n_side = b_loc.shape[1]
    n_blk = 512 if k_len > 4096 else 1024 if k_len > 1024 else 2048
    depth = 2
    grid = (n_rows // m_blk, n_side // n_blk)
    a_step = (b_loc.shape[0] // 2) // m_blk

    def a_map(r, c, meta_ref):
        return (meta_ref[0] * a_step + r if a_by_layer else r, 0)

    a_spec = pl.BlockSpec((m_blk, k_len), a_map, pipeline_mode=pl.Buffered(1 if n_rows == m_blk else 2))
    in_specs = [a_spec, pl.BlockSpec(memory_space=pl.ANY), pl.BlockSpec(memory_space=pl.ANY)]
    operands = [a_arr, b_loc, b_rcv]
    if part is not None:
        in_specs.append(pl.BlockSpec((m_blk, n_blk), lambda r, c, meta_ref: (part_off // m_blk + r, c)))
        operands.append(part)
    aliases = {}
    if out_buf is not None:
        in_specs.append(pl.BlockSpec(memory_space=pl.ANY))
        operands.append(out_buf)
        aliases = {len(operands): 0}
    return pl.pallas_call(
        functools.partial(mm_kernel, n_blk, depth, k_off, k_len, own, part is not None),
        out_shape=out_shape,
        grid_spec=pltpu.PrefetchScalarGridSpec(
            num_scalar_prefetch=1,
            grid=grid,
            in_specs=in_specs,
            out_specs=pl.BlockSpec((m_blk, n_blk), lambda r, c, meta_ref: (out_off // m_blk + r, c)),
            scratch_shapes=[pltpu.VMEM((depth, k_len, n_blk), jnp.bfloat16), pltpu.SemaphoreType.DMA((depth,))],
        ),
        input_output_aliases=aliases,
        cost_estimate=pl.CostEstimate(
            flops=2 * n_rows * k_len * n_side, bytes_accessed=2 * (n_rows + n_side) * k_len + 6 * n_rows * n_side, transcendentals=0
        ),
        compiler_params=pltpu.CompilerParams(
            dimension_semantics=("arbitrary", "arbitrary"), vmem_limit_bytes=(58 if m_blk > 512 else 28) * 1024 * 1024
        ),
        name=name,
    )(meta, *operands)


def stage_kernel(k_off, row0, meta_ref, b_loc, b_rcv, part_ref, held_ref, acc_ref, sems):
    rows = pl.ds(k_off, held_ref.shape[0])
    part_copy = pltpu.make_async_copy(part_ref.at[pl.ds(row0, acc_ref.shape[0]), :], acc_ref, sems.at[1])
    part_copy.start()

    @pl.when(meta_ref[1] == 0)
    def _():
        pltpu.make_async_copy(b_loc.at[rows, :], held_ref, sems.at[0]).start()

    @pl.when(meta_ref[1] != 0)
    def _():
        pltpu.make_async_copy(b_rcv.at[rows, :], held_ref, sems.at[0]).start()

    pltpu.make_async_copy(b_loc.at[rows, :], held_ref, sems.at[0]).wait()
    part_copy.wait()


def tail_kernel(k_off, k_len, n_blk, depth, held_off, last, box_row, row0, meta_ref, a_ref, b_loc, b_rcv, held_ref, acc_in, *refs):
    if last:
        _, out_ref, a_buf, b_buf, o_buf, a_sem, b_sems, o_sems = refs
    else:
        acc_out, a_buf, b_buf, a_sem, b_sems = refs
    (rows, _), n_side = a_buf.shape, acc_in.shape[1]
    box_rows = pl.ds(box_row, rows)
    n_steps = n_side // n_blk
    held = held_off is not None
    a_copy = pltpu.make_async_copy(a_ref, a_buf, a_sem)
    a_copy.start()

    def cols_of(blk):
        return pl.ds(pl.multiple_of(blk * n_blk, n_blk), n_blk)

    def fetch(blk, slot):
        @pl.when(meta_ref[1] == 0)
        def _():
            pltpu.make_async_copy(b_loc.at[pl.ds(k_off, k_len), cols_of(blk)], b_buf.at[slot], b_sems.at[slot]).start()

        @pl.when(meta_ref[1] != 0)
        def _():
            pltpu.make_async_copy(b_rcv.at[pl.ds(k_off, k_len), cols_of(blk)], b_buf.at[slot], b_sems.at[slot]).start()

    def store(blk):
        return pltpu.make_async_copy(o_buf.at[:, cols_of(blk)], out_ref.at[pl.ds(row0 + box_row, rows), cols_of(blk)], o_sems.at[blk])

    if not held:
        for ahead in range(depth - 1):
            fetch(ahead, ahead)
    a_copy.wait()

    def step(blk, carry):
        cols = cols_of(blk)
        if held:
            b_val = held_ref[pl.ds(held_off, k_len), cols]
        else:
            slot = lax.rem(blk, depth)

            @pl.when(blk + depth - 1 < n_steps)
            def _():
                fetch(blk + depth - 1, lax.rem(blk + depth - 1, depth))

            pltpu.make_async_copy(b_loc.at[pl.ds(k_off, k_len), pl.ds(0, n_blk)], b_buf.at[slot], b_sems.at[slot]).wait()
            b_val = b_buf[slot]
        total = acc_in[box_rows, cols] + jnp.dot(a_buf[...], b_val, preferred_element_type=jnp.float32)
        if last:
            o_buf[:, cols] = total.astype(o_buf.dtype)
            store(blk).start()
        else:
            acc_out[box_rows, cols] = total
        return carry

    lax.fori_loop(0, n_steps, step, 0, unroll=held)
    if last:
        for blk in range(n_steps):
            store(blk).wait()


SMEM = pl.BlockSpec(memory_space=pltpu.SMEM)
VMEM = pl.BlockSpec(memory_space=pltpu.VMEM)
ANY = pl.BlockSpec(memory_space=pl.ANY)


def stage_call(meta, b_loc, b_rcv, part, row0, rows):
    side, n_side = b_loc.shape
    n_held = side - HELD_FROM
    return pl.pallas_call(
        functools.partial(stage_kernel, HELD_FROM, row0),
        out_shape=(pltpu.VMEM((n_held, n_side), jnp.bfloat16), pltpu.VMEM((rows, n_side), jnp.float32)),
        in_specs=[SMEM, ANY, ANY, ANY],
        out_specs=(VMEM, VMEM),
        scratch_shapes=[pltpu.SemaphoreType.DMA((2,))],
        cost_estimate=pl.CostEstimate(flops=10**9, bytes_accessed=2 * n_held * n_side + 4 * rows * n_side, transcendentals=0),
        compiler_params=pltpu.CompilerParams(vmem_limit_bytes=1024 * 1024),
        name="stage",
    )(meta, b_loc, b_rcv, part)


def tail_call(meta, a_arr, b_loc, b_rcv, held, acc, out_buf, row0, box):
    box_row, rows, k_off, k_end = box
    k_len, n_side = k_end - k_off, acc.shape[1]
    last = out_buf is not None
    held_off = k_off - HELD_FROM if k_off >= HELD_FROM else None
    n_blk, depth = (1024 if k_len <= 1024 else 512), 3
    operands = [meta, a_arr, b_loc, b_rcv, pltpu.with_memory_space_constraint(held, pltpu.VMEM), pltpu.with_memory_space_constraint(acc, pltpu.VMEM)]
    in_specs = [SMEM, ANY, ANY, ANY, VMEM, VMEM]
    b_shape = (depth, k_len, n_blk) if held_off is None else (1, 16, 128)
    scratch = [pltpu.VMEM((rows, k_len), jnp.bfloat16), pltpu.VMEM(b_shape, jnp.bfloat16)]
    sems = [pltpu.SemaphoreType.DMA, pltpu.SemaphoreType.DMA((depth,))]
    if last:
        operands.append(out_buf)
        in_specs.append(ANY)
        out_shape, out_specs, aliases = jax.ShapeDtypeStruct(out_buf.shape, out_buf.dtype), ANY, {6: 0}
        scratch += [pltpu.VMEM((rows, n_side), jnp.bfloat16)] + sems + [pltpu.SemaphoreType.DMA((n_side // n_blk,))]
    else:
        out_shape, out_specs, aliases = pltpu.VMEM(acc.shape, jnp.float32), VMEM, {5: 0}
        scratch += sems
    return pl.pallas_call(
        functools.partial(tail_kernel, k_off, k_len, n_blk, depth, held_off, last, box_row, row0),
        out_shape=out_shape,
        in_specs=in_specs,
        out_specs=out_specs,
        scratch_shapes=scratch,
        input_output_aliases=aliases,
        cost_estimate=pl.CostEstimate(flops=2 * rows * k_len * n_side, bytes_accessed=2 * k_len * n_side, transcendentals=0),
        compiler_params=pltpu.CompilerParams(vmem_limit_bytes=10 * 1024 * 1024),
        name=f"tail_{box_row}_{k_off}",
    )(*operands)


def solution(mesh):
    swap = [(0, 1), (1, 0)]

    def local_mm(a_blk, b_blk):
        side = a_blk.shape[0]
        half = side // 2
        layer_idx = lax.axis_index("depth")
        row_idx = lax.axis_index("row")
        col_idx = lax.axis_index("col")
        meta = jnp.stack([layer_idx, (row_idx == col_idx).astype(jnp.int32)]).astype(jnp.int32)

        row_last, n_last = LAST_ROWS
        boxes = [(row0, rows, 0, side) for row0, rows in PIECES] + [(row_last + r, n, k0, k1) for r, n, k0, k1 in LAST_BOXES]
        moved = []
        for row0, rows, k0, k1 in boxes:
            part_a = lax.dynamic_slice(a_blk, (layer_idx * half + row0, k0), (rows, k1 - k0))
            moved.append(lax.ppermute(part_a, "col", swap))
            if len(moved) == 1:
                b_rcv = lax.ppermute(b_blk, "row", swap)

        call = functools.partial(mm_call, meta, b_loc=b_blk, b_rcv=b_rcv)
        part = call(
            a_blk, part=None, out_buf=None, m_blk=1024, n_rows=half, a_by_layer=True, k_off=0, k_len=side, row_off=0, part_off=0,
            out_off=0, out_shape=jax.ShapeDtypeStruct((half, side), jnp.float32), own=True, name="own_part",
        )
        out = None
        for (row0, rows), a_piece in zip(PIECES, moved):
            out = call(
                a_piece, part=part, out_buf=out, m_blk=rows, n_rows=rows, a_by_layer=False, k_off=0, k_len=side, row_off=0,
                part_off=row0, out_off=row0, out_shape=jax.ShapeDtypeStruct((half, side), jnp.bfloat16), own=False,
                name=f"piece_{row0}",
            )
        held, acc = stage_call(meta, b_blk, b_rcv, part, row_last, n_last)
        for box, a_piece in zip(LAST_BOXES, moved[len(PIECES):]):
            last = box[3] == side
            res = tail_call(meta, a_piece, b_blk, b_rcv, held, acc, out if last else None, row_last, box)
            acc, out = (acc, res) if last else (res, out)
        return out

    spec_in = P("row", "col")
    spec_out = P(("row", "depth"), "col")
    return jax.shard_map(local_mm, mesh=mesh, in_specs=(spec_in, spec_in), out_specs=spec_out, check_vma=False)
```

```python
import functools

import jax
import jax.numpy as jnp
from jax import lax
from jax.experimental import pallas as pl
from jax.experimental.pallas import tpu as pltpu
from jax.sharding import PartitionSpec as P


PIECES = ((2560, 32), (2592, 96), (0, 512), (512, 512), (1024, 512), (1536, 512), (2048, 512))
LAST_ROWS = (2688, 384)
LAST_BOXES = ((0, 384, 0, 2048), (0, 384, 2048, 4096), (0, 384, 4096, 5120), (0, 240, 5120, 6144), (240, 144, 5120, 6144))
HELD_FROM = 5120


def mm_kernel(n_blk, depth, k_off, k_len, own, with_part, meta_ref, a_ref, b_loc, b_rcv, *refs):
    if with_part:
        part_ref, refs = refs[0], refs[1:]
    out_ref, b_buf, sems = refs[-3], refs[-2], refs[-1]
    row_blk, col_blk = pl.program_id(0), pl.program_id(1)
    n_steps = pl.num_programs(0) * pl.num_programs(1)
    step = row_blk * pl.num_programs(1) + col_blk
    take_loc = meta_ref[1] == (1 if own else 0)

    def fetch(blk, slot):
        cols = pl.ds(pl.multiple_of(blk * n_blk, n_blk), n_blk)

        @pl.when(take_loc)
        def _():
            pltpu.make_async_copy(b_loc.at[pl.ds(k_off, k_len), cols], b_buf.at[slot], sems.at[slot]).start()

        @pl.when(jnp.logical_not(take_loc))
        def _():
            pltpu.make_async_copy(b_rcv.at[pl.ds(k_off, k_len), cols], b_buf.at[slot], sems.at[slot]).start()

    slot = lax.rem(step, depth)

    @pl.when(step == 0)
    def _():
        for ahead in range(depth - 1):
            fetch(ahead, ahead)

    @pl.when(step + depth - 1 < n_steps)
    def _():
        fetch(lax.rem(step + depth - 1, pl.num_programs(1)), lax.rem(step + depth - 1, depth))

    pltpu.make_async_copy(b_loc.at[pl.ds(k_off, k_len), pl.ds(0, n_blk)], b_buf.at[slot], sems.at[slot]).wait()
    prod = jnp.dot(a_ref[...], b_buf[slot], preferred_element_type=jnp.float32)
    if with_part:
        prod = part_ref[...] + prod
    out_ref[...] = prod.astype(out_ref.dtype)


def mm_call(meta, a_arr, b_loc, b_rcv, part, out_buf, *, m_blk, n_rows, a_by_layer, k_off, k_len, part_off, out_off,
            out_shape, own):
    n_side = b_loc.shape[1]
    n_blk = 512 if k_len > 4096 else 1024 if k_len > 1024 else 2048
    depth = 2
    grid = (n_rows // m_blk, n_side // n_blk)
    a_step = (b_loc.shape[0] // 2) // m_blk

    def a_map(r, c, meta_ref):
        return (meta_ref[0] * a_step + r if a_by_layer else r, 0)

    a_spec = pl.BlockSpec((m_blk, k_len), a_map, pipeline_mode=pl.Buffered(1 if n_rows == m_blk else 2))
    in_specs = [a_spec, pl.BlockSpec(memory_space=pl.ANY), pl.BlockSpec(memory_space=pl.ANY)]
    operands = [a_arr, b_loc, b_rcv]
    if part is not None:
        in_specs.append(pl.BlockSpec((m_blk, n_blk), lambda r, c, meta_ref: (part_off // m_blk + r, c)))
        operands.append(part)
    aliases = {}
    if out_buf is not None:
        in_specs.append(pl.BlockSpec(memory_space=pl.ANY))
        operands.append(out_buf)
        aliases = {len(operands): 0}
    return pl.pallas_call(
        functools.partial(mm_kernel, n_blk, depth, k_off, k_len, own, part is not None),
        out_shape=out_shape,
        grid_spec=pltpu.PrefetchScalarGridSpec(
            num_scalar_prefetch=1,
            grid=grid,
            in_specs=in_specs,
            out_specs=pl.BlockSpec((m_blk, n_blk), lambda r, c, meta_ref: (out_off // m_blk + r, c)),
            scratch_shapes=[pltpu.VMEM((depth, k_len, n_blk), jnp.bfloat16), pltpu.SemaphoreType.DMA((depth,))],
        ),
        input_output_aliases=aliases,
        cost_estimate=pl.CostEstimate(
            flops=2 * n_rows * k_len * n_side, bytes_accessed=2 * (n_rows + n_side) * k_len + 6 * n_rows * n_side, transcendentals=0
        ),
        compiler_params=pltpu.CompilerParams(
            dimension_semantics=("arbitrary", "arbitrary"), vmem_limit_bytes=(58 if m_blk > 512 else 28) * 1024 * 1024
        ),
    )(meta, *operands)


def stage_kernel(k_off, row0, meta_ref, b_loc, b_rcv, part_ref, held_ref, acc_ref, meta_out, sems):
    rows = pl.ds(k_off, held_ref.shape[0])
    part_copy = pltpu.make_async_copy(part_ref.at[pl.ds(row0, acc_ref.shape[0]), :], acc_ref, sems.at[1])
    part_copy.start()
    meta_out[0] = meta_ref[0]
    meta_out[1] = meta_ref[1]

    @pl.when(meta_ref[1] == 0)
    def _():
        pltpu.make_async_copy(b_loc.at[rows, :], held_ref, sems.at[0]).start()

    @pl.when(meta_ref[1] != 0)
    def _():
        pltpu.make_async_copy(b_rcv.at[rows, :], held_ref, sems.at[0]).start()

    pltpu.make_async_copy(b_loc.at[rows, :], held_ref, sems.at[0]).wait()
    part_copy.wait()


def tail_kernel(k_off, k_len, n_blk, depth, held_off, last, box_row, row0, meta_ref, a_ref, b_loc, b_rcv, held_ref, acc_in, *refs):
    if last:
        _, out_ref, a_buf, b_buf, o_buf, a_sem, b_sems, o_sems = refs
    else:
        acc_out, a_buf, b_buf, a_sem, b_sems = refs
    (rows, _), n_side = a_buf.shape, acc_in.shape[1]
    box_rows = pl.ds(box_row, rows)
    n_steps = n_side // n_blk
    held = held_off is not None
    a_copy = pltpu.make_async_copy(a_ref, a_buf, a_sem)
    a_copy.start()

    def cols_of(blk):
        return pl.ds(pl.multiple_of(blk * n_blk, n_blk), n_blk)

    def fetch(blk, slot):
        @pl.when(meta_ref[1] == 0)
        def _():
            pltpu.make_async_copy(b_loc.at[pl.ds(k_off, k_len), cols_of(blk)], b_buf.at[slot], b_sems.at[slot]).start()

        @pl.when(meta_ref[1] != 0)
        def _():
            pltpu.make_async_copy(b_rcv.at[pl.ds(k_off, k_len), cols_of(blk)], b_buf.at[slot], b_sems.at[slot]).start()

    def store(blk):
        return pltpu.make_async_copy(o_buf.at[:, cols_of(blk)], out_ref.at[pl.ds(row0 + box_row, rows), cols_of(blk)], o_sems.at[blk])

    if not held:
        for ahead in range(depth - 1):
            fetch(ahead, ahead)
    a_copy.wait()

    def step(blk, carry):
        cols = cols_of(blk)
        if held:
            b_val = held_ref[pl.ds(held_off, k_len), cols]
        else:
            slot = lax.rem(blk, depth)

            @pl.when(blk + depth - 1 < n_steps)
            def _():
                fetch(blk + depth - 1, lax.rem(blk + depth - 1, depth))

            pltpu.make_async_copy(b_loc.at[pl.ds(k_off, k_len), pl.ds(0, n_blk)], b_buf.at[slot], b_sems.at[slot]).wait()
            b_val = b_buf[slot]
        total = acc_in[box_rows, cols] + jnp.dot(a_buf[...], b_val, preferred_element_type=jnp.float32)
        if last:
            o_buf[:, cols] = total.astype(o_buf.dtype)
            store(blk).start()
        else:
            acc_out[box_rows, cols] = total
        return carry

    lax.fori_loop(0, n_steps, step, 0, unroll=held)
    if last:
        for blk in range(n_steps):
            store(blk).wait()


SMEM = pl.BlockSpec(memory_space=pltpu.SMEM)
VMEM = pl.BlockSpec(memory_space=pltpu.VMEM)
ANY = pl.BlockSpec(memory_space=pl.ANY)


def stage_call(meta, b_loc, b_rcv, part, row0, rows):
    side, n_side = b_loc.shape
    n_held = side - HELD_FROM
    return pl.pallas_call(
        functools.partial(stage_kernel, HELD_FROM, row0),
        out_shape=(pltpu.VMEM((n_held, n_side), jnp.bfloat16), pltpu.VMEM((rows, n_side), jnp.float32), jax.ShapeDtypeStruct((2,), jnp.int32)),
        in_specs=[SMEM, ANY, ANY, ANY],
        out_specs=(VMEM, VMEM, SMEM),
        scratch_shapes=[pltpu.SemaphoreType.DMA((2,))],
        cost_estimate=pl.CostEstimate(flops=10**9, bytes_accessed=2 * n_held * n_side + 4 * rows * n_side, transcendentals=0),
        compiler_params=pltpu.CompilerParams(vmem_limit_bytes=1024 * 1024),
        name="stage",
    )(meta, b_loc, b_rcv, part)


def tail_call(meta, a_arr, b_loc, b_rcv, held, acc, out_buf, row0, box):
    box_row, rows, k_off, k_end = box
    k_len, n_side = k_end - k_off, acc.shape[1]
    last = out_buf is not None
    held_off = k_off - HELD_FROM if k_off >= HELD_FROM else None
    n_blk, depth = (1024 if k_len <= 1024 else 512), 3
    operands = [meta, a_arr, b_loc, b_rcv, pltpu.with_memory_space_constraint(held, pltpu.VMEM), pltpu.with_memory_space_constraint(acc, pltpu.VMEM)]
    in_specs = [SMEM, ANY, ANY, ANY, VMEM, VMEM]
    b_shape = (depth, k_len, n_blk) if held_off is None else (1, 16, 128)
    scratch = [pltpu.VMEM((rows, k_len), jnp.bfloat16), pltpu.VMEM(b_shape, jnp.bfloat16)]
    sems = [pltpu.SemaphoreType.DMA, pltpu.SemaphoreType.DMA((depth,))]
    if last:
        operands.append(out_buf)
        in_specs.append(ANY)
        out_shape, out_specs, aliases = jax.ShapeDtypeStruct(out_buf.shape, out_buf.dtype), ANY, {6: 0}
        scratch += [pltpu.VMEM((rows, n_side), jnp.bfloat16)] + sems + [pltpu.SemaphoreType.DMA((n_side // n_blk,))]
    else:
        out_shape, out_specs, aliases = pltpu.VMEM(acc.shape, jnp.float32), VMEM, {5: 0}
        scratch += sems
    return pl.pallas_call(
        functools.partial(tail_kernel, k_off, k_len, n_blk, depth, held_off, last, box_row, row0),
        out_shape=out_shape,
        in_specs=in_specs,
        out_specs=out_specs,
        scratch_shapes=scratch,
        input_output_aliases=aliases,
        cost_estimate=pl.CostEstimate(flops=2 * rows * k_len * n_side, bytes_accessed=2 * k_len * n_side, transcendentals=0),
        compiler_params=pltpu.CompilerParams(vmem_limit_bytes=10 * 1024 * 1024),
    )(*operands)


def solution(mesh):
    swap = [(0, 1), (1, 0)]

    def local_mm(a_blk, b_blk):
        side = a_blk.shape[0]
        half = side // 2
        layer_idx = lax.axis_index("depth")
        row_idx = lax.axis_index("row")
        col_idx = lax.axis_index("col")
        meta = jnp.stack([layer_idx, (row_idx == col_idx).astype(jnp.int32)]).astype(jnp.int32)

        row_last, n_last = LAST_ROWS
        boxes = [(row0, rows, 0, side) for row0, rows in PIECES] + [(row_last + r, n, k0, k1) for r, n, k0, k1 in LAST_BOXES]
        moved = []
        for row0, rows, k0, k1 in boxes:
            part_a = lax.dynamic_slice(a_blk, (layer_idx * half + row0, k0), (rows, k1 - k0))
            moved.append(lax.ppermute(part_a, "col", swap))
        b_rcv = lax.ppermute(b_blk, "row", swap)

        part = mm_call(
            meta, a_blk, b_blk, b_rcv, None, None, m_blk=1024, n_rows=half, a_by_layer=True, k_off=0, k_len=side,
            part_off=0, out_off=0, out_shape=jax.ShapeDtypeStruct((half, side), jnp.float32), own=True,
        )
        out = None
        for (row0, rows), a_piece in zip(PIECES, moved):
            if row0 == PIECES[-1][0]:
                held, acc, meta = stage_call(meta, b_blk, b_rcv, part, row_last, n_last)
            out = mm_call(
                meta, a_piece, b_blk, b_rcv, part, out, m_blk=rows, n_rows=rows, a_by_layer=False, k_off=0, k_len=side,
                part_off=row0, out_off=row0, out_shape=jax.ShapeDtypeStruct((half, side), jnp.bfloat16), own=False,
            )
        for box, a_piece in zip(LAST_BOXES, moved[len(PIECES):]):
            last = box[3] == side
            res = tail_call(meta, a_piece, b_blk, b_rcv, held, acc, out if last else None, row_last, box)
            acc, out = (acc, res) if last else (res, out)
        return out

    spec_in = P("row", "col")
    spec_out = P(("row", "depth"), "col")
    return jax.shard_map(local_mm, mesh=mesh, in_specs=(spec_in, spec_in), out_specs=spec_out, check_vma=False)
```

```python
import functools

import jax
import jax.numpy as jnp
from jax import lax
from jax.experimental import pallas as pl
from jax.experimental.pallas import tpu as pltpu
from jax.sharding import PartitionSpec as P


PIECES = ((2560, 32), (2592, 96), (0, 512), (512, 512), (1024, 512), (1536, 512), (2048, 512))
LAST_ROWS = (2688, 384)
LAST_BOXES = ((0, 384, 0, 2048), (0, 384, 2048, 4096), (0, 384, 4096, 5120), (0, 240, 5120, 6144), (240, 144, 5120, 6144))
HELD_FROM = 5120
END_COLUMNS = (1536,) * 3 + (1024, 512)


def mm_kernel(n_blk, depth, k_off, k_len, own, with_part, meta_ref, a_ref, b_loc, b_rcv, *refs):
    if with_part:
        part_ref, refs = refs[0], refs[1:]
    out_ref, b_buf, sems = refs[-3], refs[-2], refs[-1]
    row_blk, col_blk = pl.program_id(0), pl.program_id(1)
    n_steps = pl.num_programs(0) * pl.num_programs(1)
    step = row_blk * pl.num_programs(1) + col_blk
    take_loc = meta_ref[1] == (1 if own else 0)

    def fetch(blk, slot):
        cols = pl.ds(pl.multiple_of(blk * n_blk, n_blk), n_blk)

        @pl.when(take_loc)
        def _():
            pltpu.make_async_copy(b_loc.at[pl.ds(k_off, k_len), cols], b_buf.at[slot], sems.at[slot]).start()

        @pl.when(jnp.logical_not(take_loc))
        def _():
            pltpu.make_async_copy(b_rcv.at[pl.ds(k_off, k_len), cols], b_buf.at[slot], sems.at[slot]).start()

    slot = lax.rem(step, depth)

    @pl.when(step == 0)
    def _():
        for ahead in range(depth - 1):
            fetch(ahead, ahead)

    @pl.when(step + depth - 1 < n_steps)
    def _():
        fetch(lax.rem(step + depth - 1, pl.num_programs(1)), lax.rem(step + depth - 1, depth))

    pltpu.make_async_copy(b_loc.at[pl.ds(k_off, k_len), pl.ds(0, n_blk)], b_buf.at[slot], sems.at[slot]).wait()
    prod = jnp.dot(a_ref[...], b_buf[slot], preferred_element_type=jnp.float32)
    if with_part:
        prod = part_ref[...] + prod
    out_ref[...] = prod.astype(out_ref.dtype)


def mm_call(meta, a_arr, b_loc, b_rcv, part, out_buf, *, m_blk, n_rows, a_by_layer, k_off, k_len, part_off, out_off,
            out_shape, own):
    n_side = b_loc.shape[1]
    n_blk = 512 if k_len > 4096 else 1024 if k_len > 1024 else 2048
    depth = 2
    grid = (n_rows // m_blk, n_side // n_blk)
    a_step = (b_loc.shape[0] // 2) // m_blk

    def a_map(r, c, meta_ref):
        return (meta_ref[0] * a_step + r if a_by_layer else r, 0)

    a_spec = pl.BlockSpec((m_blk, k_len), a_map, pipeline_mode=pl.Buffered(1 if n_rows == m_blk else 2))
    in_specs = [a_spec, pl.BlockSpec(memory_space=pl.ANY), pl.BlockSpec(memory_space=pl.ANY)]
    operands = [a_arr, b_loc, b_rcv]
    if part is not None:
        in_specs.append(pl.BlockSpec((m_blk, n_blk), lambda r, c, meta_ref: (part_off // m_blk + r, c)))
        operands.append(part)
    aliases = {}
    if out_buf is not None:
        in_specs.append(pl.BlockSpec(memory_space=pl.ANY))
        operands.append(out_buf)
        aliases = {len(operands): 0}
    return pl.pallas_call(
        functools.partial(mm_kernel, n_blk, depth, k_off, k_len, own, part is not None),
        out_shape=out_shape,
        grid_spec=pltpu.PrefetchScalarGridSpec(
            num_scalar_prefetch=1,
            grid=grid,
            in_specs=in_specs,
            out_specs=pl.BlockSpec((m_blk, n_blk), lambda r, c, meta_ref: (out_off // m_blk + r, c)),
            scratch_shapes=[pltpu.VMEM((depth, k_len, n_blk), jnp.bfloat16), pltpu.SemaphoreType.DMA((depth,))],
        ),
        input_output_aliases=aliases,
        cost_estimate=pl.CostEstimate(
            flops=2 * n_rows * k_len * n_side, bytes_accessed=2 * (n_rows + n_side) * k_len + 6 * n_rows * n_side, transcendentals=0
        ),
        compiler_params=pltpu.CompilerParams(
            dimension_semantics=("arbitrary", "arbitrary"), vmem_limit_bytes=(58 if m_blk > 512 else 28) * 1024 * 1024
        ),
    )(meta, *operands)


def stage_kernel(k_off, row0, meta_ref, b_loc, b_rcv, part_ref, held_ref, acc_ref, meta_out, sems):
    rows = pl.ds(k_off, held_ref.shape[0])
    part_copy = pltpu.make_async_copy(part_ref.at[pl.ds(row0, acc_ref.shape[0]), :], acc_ref, sems.at[1])
    part_copy.start()
    meta_out[0] = meta_ref[0]
    meta_out[1] = meta_ref[1]

    @pl.when(meta_ref[1] == 0)
    def _():
        pltpu.make_async_copy(b_loc.at[rows, :], held_ref, sems.at[0]).start()

    @pl.when(meta_ref[1] != 0)
    def _():
        pltpu.make_async_copy(b_rcv.at[rows, :], held_ref, sems.at[0]).start()

    pltpu.make_async_copy(b_loc.at[rows, :], held_ref, sems.at[0]).wait()
    part_copy.wait()


def tail_kernel(k_off, k_len, n_blk, depth, box_row, meta_ref, a_ref, b_loc, b_rcv, acc_in, acc_out, a_buf, b_buf, a_sem, b_sems):
    (rows, _), n_side = a_buf.shape, acc_in.shape[1]
    box_rows = pl.ds(box_row, rows)
    n_steps = n_side // n_blk
    a_copy = pltpu.make_async_copy(a_ref, a_buf, a_sem)
    a_copy.start()

    def cols_of(blk):
        return pl.ds(pl.multiple_of(blk * n_blk, n_blk), n_blk)

    def fetch(blk, slot):
        @pl.when(meta_ref[1] == 0)
        def _():
            pltpu.make_async_copy(b_loc.at[pl.ds(k_off, k_len), cols_of(blk)], b_buf.at[slot], b_sems.at[slot]).start()

        @pl.when(meta_ref[1] != 0)
        def _():
            pltpu.make_async_copy(b_rcv.at[pl.ds(k_off, k_len), cols_of(blk)], b_buf.at[slot], b_sems.at[slot]).start()

    for ahead in range(depth - 1):
        fetch(ahead, ahead)
    a_copy.wait()

    def step(blk, carry):
        slot = lax.rem(blk, depth)

        @pl.when(blk + depth - 1 < n_steps)
        def _():
            fetch(blk + depth - 1, lax.rem(blk + depth - 1, depth))

        pltpu.make_async_copy(b_loc.at[pl.ds(k_off, k_len), pl.ds(0, n_blk)], b_buf.at[slot], b_sems.at[slot]).wait()
        cols = cols_of(blk)
        acc_out[box_rows, cols] = acc_in[box_rows, cols] + jnp.dot(a_buf[...], b_buf[slot], preferred_element_type=jnp.float32)
        return carry

    lax.fori_loop(0, n_steps, step, 0)


def end_kernel(held_off, n_blks, box_row, row0, a_ref, held_ref, acc_ref, _, out_ref, a_buf, o_buf, a_sem, o_sems):
    rows, k_len = a_buf.shape
    box_rows = pl.ds(box_row, rows)
    a_copy = pltpu.make_async_copy(a_ref, a_buf, a_sem)
    a_copy.start()
    a_copy.wait()
    stores, first = [], 0
    for blk, n_blk in enumerate(n_blks):
        cols = pl.ds(first, n_blk)
        total = acc_ref[box_rows, cols] + jnp.dot(
            a_buf[...], held_ref[pl.ds(held_off, k_len), cols], preferred_element_type=jnp.float32
        )
        o_buf[:, cols] = total.astype(o_buf.dtype)
        stores.append(pltpu.make_async_copy(o_buf.at[:, cols], out_ref.at[pl.ds(row0 + box_row, rows), cols], o_sems.at[blk]))
        stores[-1].start()
        first += n_blk
    for copy in stores:
        copy.wait()


SMEM = pl.BlockSpec(memory_space=pltpu.SMEM)
VMEM = pl.BlockSpec(memory_space=pltpu.VMEM)
ANY = pl.BlockSpec(memory_space=pl.ANY)


def stage_call(meta, b_loc, b_rcv, part, row0, rows):
    side, n_side = b_loc.shape
    n_held = side - HELD_FROM
    return pl.pallas_call(
        functools.partial(stage_kernel, HELD_FROM, row0),
        out_shape=(pltpu.VMEM((n_held, n_side), jnp.bfloat16), pltpu.VMEM((rows, n_side), jnp.float32), jax.ShapeDtypeStruct((2,), jnp.int32)),
        in_specs=[SMEM, ANY, ANY, ANY],
        out_specs=(VMEM, VMEM, SMEM),
        scratch_shapes=[pltpu.SemaphoreType.DMA((2,))],
        cost_estimate=pl.CostEstimate(flops=10**9, bytes_accessed=2 * n_held * n_side + 4 * rows * n_side, transcendentals=0),
        compiler_params=pltpu.CompilerParams(vmem_limit_bytes=1024 * 1024),
        name="stage",
    )(meta, b_loc, b_rcv, part)


def tail_call(meta, a_arr, b_loc, b_rcv, acc, box):
    box_row, rows, k_off, k_end = box
    k_len, n_side = k_end - k_off, acc.shape[1]
    n_blk, depth = (1024 if k_len <= 1024 else 512), 3
    return pl.pallas_call(
        functools.partial(tail_kernel, k_off, k_len, n_blk, depth, box_row),
        out_shape=pltpu.VMEM(acc.shape, jnp.float32),
        in_specs=[SMEM, ANY, ANY, ANY, VMEM],
        out_specs=VMEM,
        scratch_shapes=[
            pltpu.VMEM((rows, k_len), jnp.bfloat16),
            pltpu.VMEM((depth, k_len, n_blk), jnp.bfloat16),
            pltpu.SemaphoreType.DMA,
            pltpu.SemaphoreType.DMA((depth,)),
        ],
        input_output_aliases={4: 0},
        cost_estimate=pl.CostEstimate(flops=2 * rows * k_len * n_side, bytes_accessed=2 * k_len * n_side, transcendentals=0),
        compiler_params=pltpu.CompilerParams(vmem_limit_bytes=10 * 1024 * 1024),
    )(meta, a_arr, b_loc, b_rcv, pltpu.with_memory_space_constraint(acc, pltpu.VMEM))


def end_call(a_arr, held, acc, out_buf, row0, box):
    box_row, rows, k_off, k_end = box
    k_len, n_side = k_end - k_off, acc.shape[1]
    return pl.pallas_call(
        functools.partial(end_kernel, k_off - HELD_FROM, END_COLUMNS, box_row, row0),
        out_shape=jax.ShapeDtypeStruct(out_buf.shape, out_buf.dtype),
        in_specs=[ANY, VMEM, VMEM, ANY],
        out_specs=ANY,
        scratch_shapes=[
            pltpu.VMEM((rows, k_len), jnp.bfloat16),
            pltpu.VMEM((rows, n_side), jnp.bfloat16),
            pltpu.SemaphoreType.DMA,
            pltpu.SemaphoreType.DMA((len(END_COLUMNS),)),
        ],
        input_output_aliases={3: 0},
        cost_estimate=pl.CostEstimate(flops=2 * rows * k_len * n_side, bytes_accessed=2 * rows * n_side, transcendentals=0),
        compiler_params=pltpu.CompilerParams(vmem_limit_bytes=10 * 1024 * 1024),
    )(a_arr, pltpu.with_memory_space_constraint(held, pltpu.VMEM), pltpu.with_memory_space_constraint(acc, pltpu.VMEM), out_buf)


def solution(mesh):
    swap = [(0, 1), (1, 0)]

    def local_mm(a_blk, b_blk):
        side = a_blk.shape[0]
        half = side // 2
        layer_idx = lax.axis_index("depth")
        row_idx = lax.axis_index("row")
        col_idx = lax.axis_index("col")
        meta = jnp.stack([layer_idx, (row_idx == col_idx).astype(jnp.int32)]).astype(jnp.int32)

        row_last, n_last = LAST_ROWS
        boxes = [(row0, rows, 0, side) for row0, rows in PIECES] + [(row_last + r, n, k0, k1) for r, n, k0, k1 in LAST_BOXES]
        moved = []
        for row0, rows, k0, k1 in boxes:
            part_a = lax.dynamic_slice(a_blk, (layer_idx * half + row0, k0), (rows, k1 - k0))
            moved.append(lax.ppermute(part_a, "col", swap))
        b_rcv = lax.ppermute(b_blk, "row", swap)

        part = mm_call(
            meta, a_blk, b_blk, b_rcv, None, None, m_blk=1024, n_rows=half, a_by_layer=True, k_off=0, k_len=side,
            part_off=0, out_off=0, out_shape=jax.ShapeDtypeStruct((half, side), jnp.float32), own=True,
        )
        out = None
        for (row0, rows), a_piece in zip(PIECES, moved):
            if row0 == PIECES[-1][0]:
                held, acc, meta = stage_call(meta, b_blk, b_rcv, part, row_last, n_last)
            out = mm_call(
                meta, a_piece, b_blk, b_rcv, part, out, m_blk=rows, n_rows=rows, a_by_layer=False, k_off=0, k_len=side,
                part_off=row0, out_off=row0, out_shape=jax.ShapeDtypeStruct((half, side), jnp.bfloat16), own=False,
            )
        for box, a_piece in zip(LAST_BOXES, moved[len(PIECES):]):
            if box[2] < HELD_FROM:
                acc = tail_call(meta, a_piece, b_blk, b_rcv, acc, box)
            else:
                out = end_call(a_piece, held, acc, out, row_last, box)
        return out

    spec_in = P("row", "col")
    spec_out = P(("row", "depth"), "col")
    return jax.shard_map(local_mm, mesh=mesh, in_specs=(spec_in, spec_in), out_specs=spec_out, check_vma=False)
```

```python
import functools

import jax
import jax.numpy as jnp
from jax import lax
from jax.experimental import pallas as pl
from jax.experimental.pallas import tpu as pltpu
from jax.sharding import PartitionSpec as P


PIECES = ((2560, 32), (2592, 96), (0, 512), (512, 512), (1024, 512), (1536, 512), (2048, 512))
LAST_ROWS = (2688, 384)
LAST_BOXES = (
    (0, 384, 0, 2048),
    (0, 384, 2048, 3584),
    (0, 384, 3584, 4608),
    (0, 384, 4608, 5120),
    (0, 176, 5120, 6144),
    (176, 112, 5120, 6144),
    (288, 96, 5120, 6144),
)
HELD_FROM = 5120
END_COLUMNS = (1536,) * 3 + (1024, 512)


def mm_kernel(n_blk, depth, k_off, k_len, own, with_part, meta_ref, a_ref, b_loc, b_rcv, *refs):
    if with_part:
        part_ref, refs = refs[0], refs[1:]
    out_ref, b_buf, sems = refs[-3], refs[-2], refs[-1]
    row_blk, col_blk = pl.program_id(0), pl.program_id(1)
    n_steps = pl.num_programs(0) * pl.num_programs(1)
    step = row_blk * pl.num_programs(1) + col_blk
    take_loc = meta_ref[1] == (1 if own else 0)

    def fetch(blk, slot):
        cols = pl.ds(pl.multiple_of(blk * n_blk, n_blk), n_blk)

        @pl.when(take_loc)
        def _():
            pltpu.make_async_copy(b_loc.at[pl.ds(k_off, k_len), cols], b_buf.at[slot], sems.at[slot]).start()

        @pl.when(jnp.logical_not(take_loc))
        def _():
            pltpu.make_async_copy(b_rcv.at[pl.ds(k_off, k_len), cols], b_buf.at[slot], sems.at[slot]).start()

    slot = lax.rem(step, depth)

    @pl.when(step == 0)
    def _():
        for ahead in range(depth - 1):
            fetch(ahead, ahead)

    @pl.when(step + depth - 1 < n_steps)
    def _():
        fetch(lax.rem(step + depth - 1, pl.num_programs(1)), lax.rem(step + depth - 1, depth))

    pltpu.make_async_copy(b_loc.at[pl.ds(k_off, k_len), pl.ds(0, n_blk)], b_buf.at[slot], sems.at[slot]).wait()
    prod = jnp.dot(a_ref[...], b_buf[slot], preferred_element_type=jnp.float32)
    if with_part:
        prod = part_ref[...] + prod
    out_ref[...] = prod.astype(out_ref.dtype)


def mm_call(meta, a_arr, b_loc, b_rcv, part, out_buf, *, m_blk, n_rows, a_by_layer, k_off, k_len, part_off, out_off,
            out_shape, own):
    n_side = b_loc.shape[1]
    n_blk = 512 if k_len > 4096 else 1024 if k_len > 1024 else 2048
    depth = 2
    grid = (n_rows // m_blk, n_side // n_blk)
    a_step = (b_loc.shape[0] // 2) // m_blk

    def a_map(r, c, meta_ref):
        return (meta_ref[0] * a_step + r if a_by_layer else r, 0)

    a_spec = pl.BlockSpec((m_blk, k_len), a_map, pipeline_mode=pl.Buffered(1 if n_rows == m_blk else 2))
    in_specs = [a_spec, pl.BlockSpec(memory_space=pl.ANY), pl.BlockSpec(memory_space=pl.ANY)]
    operands = [a_arr, b_loc, b_rcv]
    if part is not None:
        in_specs.append(pl.BlockSpec((m_blk, n_blk), lambda r, c, meta_ref: (part_off // m_blk + r, c)))
        operands.append(part)
    aliases = {}
    if out_buf is not None:
        in_specs.append(pl.BlockSpec(memory_space=pl.ANY))
        operands.append(out_buf)
        aliases = {len(operands): 0}
    return pl.pallas_call(
        functools.partial(mm_kernel, n_blk, depth, k_off, k_len, own, part is not None),
        out_shape=out_shape,
        grid_spec=pltpu.PrefetchScalarGridSpec(
            num_scalar_prefetch=1,
            grid=grid,
            in_specs=in_specs,
            out_specs=pl.BlockSpec((m_blk, n_blk), lambda r, c, meta_ref: (out_off // m_blk + r, c)),
            scratch_shapes=[pltpu.VMEM((depth, k_len, n_blk), jnp.bfloat16), pltpu.SemaphoreType.DMA((depth,))],
        ),
        input_output_aliases=aliases,
        cost_estimate=pl.CostEstimate(
            flops=2 * n_rows * k_len * n_side, bytes_accessed=2 * (n_rows + n_side) * k_len + 6 * n_rows * n_side, transcendentals=0
        ),
        compiler_params=pltpu.CompilerParams(
            dimension_semantics=("arbitrary", "arbitrary"), vmem_limit_bytes=(58 if m_blk > 512 else 28) * 1024 * 1024
        ),
    )(meta, *operands)


def stage_kernel(k_off, row0, meta_ref, b_loc, b_rcv, part_ref, held_ref, acc_ref, meta_out, sems):
    rows = pl.ds(k_off, held_ref.shape[0])
    part_copy = pltpu.make_async_copy(part_ref.at[pl.ds(row0, acc_ref.shape[0]), :], acc_ref, sems.at[1])
    part_copy.start()
    meta_out[0] = meta_ref[0]
    meta_out[1] = meta_ref[1]

    @pl.when(meta_ref[1] == 0)
    def _():
        pltpu.make_async_copy(b_loc.at[rows, :], held_ref, sems.at[0]).start()

    @pl.when(meta_ref[1] != 0)
    def _():
        pltpu.make_async_copy(b_rcv.at[rows, :], held_ref, sems.at[0]).start()

    pltpu.make_async_copy(b_loc.at[rows, :], held_ref, sems.at[0]).wait()
    part_copy.wait()


def tail_kernel(k_off, k_len, n_blk, depth, box_row, meta_ref, a_ref, b_loc, b_rcv, acc_in, acc_out, a_buf, b_buf, a_sem, b_sems):
    (rows, _), n_side = a_buf.shape, acc_in.shape[1]
    box_rows = pl.ds(box_row, rows)
    n_steps = n_side // n_blk
    a_copy = pltpu.make_async_copy(a_ref, a_buf, a_sem)
    a_copy.start()

    def cols_of(blk):
        return pl.ds(pl.multiple_of(blk * n_blk, n_blk), n_blk)

    def fetch(blk, slot):
        @pl.when(meta_ref[1] == 0)
        def _():
            pltpu.make_async_copy(b_loc.at[pl.ds(k_off, k_len), cols_of(blk)], b_buf.at[slot], b_sems.at[slot]).start()

        @pl.when(meta_ref[1] != 0)
        def _():
            pltpu.make_async_copy(b_rcv.at[pl.ds(k_off, k_len), cols_of(blk)], b_buf.at[slot], b_sems.at[slot]).start()

    for ahead in range(depth - 1):
        fetch(ahead, ahead)
    a_copy.wait()

    def step(blk, carry):
        slot = lax.rem(blk, depth)

        @pl.when(blk + depth - 1 < n_steps)
        def _():
            fetch(blk + depth - 1, lax.rem(blk + depth - 1, depth))

        pltpu.make_async_copy(b_loc.at[pl.ds(k_off, k_len), pl.ds(0, n_blk)], b_buf.at[slot], b_sems.at[slot]).wait()
        cols = cols_of(blk)
        acc_out[box_rows, cols] = acc_in[box_rows, cols] + jnp.dot(a_buf[...], b_buf[slot], preferred_element_type=jnp.float32)
        return carry

    lax.fori_loop(0, n_steps, step, 0)


def end_kernel(held_off, n_blks, box_row, row0, a_ref, held_ref, acc_ref, _, out_ref, a_buf, o_buf, a_sem, o_sems):
    rows, k_len = a_buf.shape
    box_rows = pl.ds(box_row, rows)
    a_copy = pltpu.make_async_copy(a_ref, a_buf, a_sem)
    a_copy.start()
    a_copy.wait()
    stores, first = [], 0
    for blk, n_blk in enumerate(n_blks):
        cols = pl.ds(first, n_blk)
        total = acc_ref[box_rows, cols] + jnp.dot(
            a_buf[...], held_ref[pl.ds(held_off, k_len), cols], preferred_element_type=jnp.float32
        )
        o_buf[:, cols] = total.astype(o_buf.dtype)
        stores.append(pltpu.make_async_copy(o_buf.at[:, cols], out_ref.at[pl.ds(row0 + box_row, rows), cols], o_sems.at[blk]))
        stores[-1].start()
        first += n_blk
    for copy in stores:
        copy.wait()


SMEM = pl.BlockSpec(memory_space=pltpu.SMEM)
VMEM = pl.BlockSpec(memory_space=pltpu.VMEM)
ANY = pl.BlockSpec(memory_space=pl.ANY)


def stage_call(meta, b_loc, b_rcv, part, row0, rows):
    side, n_side = b_loc.shape
    n_held = side - HELD_FROM
    return pl.pallas_call(
        functools.partial(stage_kernel, HELD_FROM, row0),
        out_shape=(pltpu.VMEM((n_held, n_side), jnp.bfloat16), pltpu.VMEM((rows, n_side), jnp.float32), jax.ShapeDtypeStruct((2,), jnp.int32)),
        in_specs=[SMEM, ANY, ANY, ANY],
        out_specs=(VMEM, VMEM, SMEM),
        scratch_shapes=[pltpu.SemaphoreType.DMA((2,))],
        cost_estimate=pl.CostEstimate(flops=10**9, bytes_accessed=2 * n_held * n_side + 4 * rows * n_side, transcendentals=0),
        compiler_params=pltpu.CompilerParams(vmem_limit_bytes=1024 * 1024),
        name="stage",
    )(meta, b_loc, b_rcv, part)


def tail_call(meta, a_arr, b_loc, b_rcv, acc, box):
    box_row, rows, k_off, k_end = box
    k_len, n_side = k_end - k_off, acc.shape[1]
    n_blk, depth = (1024 if k_len <= 1024 else 512), 3
    return pl.pallas_call(
        functools.partial(tail_kernel, k_off, k_len, n_blk, depth, box_row),
        out_shape=pltpu.VMEM(acc.shape, jnp.float32),
        in_specs=[SMEM, ANY, ANY, ANY, VMEM],
        out_specs=VMEM,
        scratch_shapes=[
            pltpu.VMEM((rows, k_len), jnp.bfloat16),
            pltpu.VMEM((depth, k_len, n_blk), jnp.bfloat16),
            pltpu.SemaphoreType.DMA,
            pltpu.SemaphoreType.DMA((depth,)),
        ],
        input_output_aliases={4: 0},
        cost_estimate=pl.CostEstimate(flops=2 * rows * k_len * n_side, bytes_accessed=2 * k_len * n_side, transcendentals=0),
        compiler_params=pltpu.CompilerParams(vmem_limit_bytes=10 * 1024 * 1024),
    )(meta, a_arr, b_loc, b_rcv, pltpu.with_memory_space_constraint(acc, pltpu.VMEM))


def end_call(a_arr, held, acc, out_buf, row0, box):
    box_row, rows, k_off, k_end = box
    k_len, n_side = k_end - k_off, acc.shape[1]
    return pl.pallas_call(
        functools.partial(end_kernel, k_off - HELD_FROM, END_COLUMNS, box_row, row0),
        out_shape=jax.ShapeDtypeStruct(out_buf.shape, out_buf.dtype),
        in_specs=[ANY, VMEM, VMEM, ANY],
        out_specs=ANY,
        scratch_shapes=[
            pltpu.VMEM((rows, k_len), jnp.bfloat16),
            pltpu.VMEM((rows, n_side), jnp.bfloat16),
            pltpu.SemaphoreType.DMA,
            pltpu.SemaphoreType.DMA((len(END_COLUMNS),)),
        ],
        input_output_aliases={3: 0},
        cost_estimate=pl.CostEstimate(flops=2 * rows * k_len * n_side, bytes_accessed=2 * rows * n_side, transcendentals=0),
        compiler_params=pltpu.CompilerParams(vmem_limit_bytes=10 * 1024 * 1024),
    )(a_arr, pltpu.with_memory_space_constraint(held, pltpu.VMEM), pltpu.with_memory_space_constraint(acc, pltpu.VMEM), out_buf)


def solution(mesh):
    swap = [(0, 1), (1, 0)]

    def local_mm(a_blk, b_blk):
        side = a_blk.shape[0]
        half = side // 2
        layer_idx = lax.axis_index("depth")
        row_idx = lax.axis_index("row")
        col_idx = lax.axis_index("col")
        meta = jnp.stack([layer_idx, (row_idx == col_idx).astype(jnp.int32)]).astype(jnp.int32)

        row_last, n_last = LAST_ROWS
        boxes = [(row0, rows, 0, side) for row0, rows in PIECES] + [(row_last + r, n, k0, k1) for r, n, k0, k1 in LAST_BOXES]
        moved = []
        for row0, rows, k0, k1 in boxes:
            part_a = lax.dynamic_slice(a_blk, (layer_idx * half + row0, k0), (rows, k1 - k0))
            moved.append(lax.ppermute(part_a, "col", swap))
        b_rcv = lax.ppermute(b_blk, "row", swap)

        part = mm_call(
            meta, a_blk, b_blk, b_rcv, None, None, m_blk=1024, n_rows=half, a_by_layer=True, k_off=0, k_len=side,
            part_off=0, out_off=0, out_shape=jax.ShapeDtypeStruct((half, side), jnp.float32), own=True,
        )
        out = None
        for (row0, rows), a_piece in zip(PIECES, moved):
            if row0 == PIECES[-1][0]:
                held, acc, meta = stage_call(meta, b_blk, b_rcv, part, row_last, n_last)
            out = mm_call(
                meta, a_piece, b_blk, b_rcv, part, out, m_blk=rows, n_rows=rows, a_by_layer=False, k_off=0, k_len=side,
                part_off=row0, out_off=row0, out_shape=jax.ShapeDtypeStruct((half, side), jnp.bfloat16), own=False,
            )
        for box, a_piece in zip(LAST_BOXES, moved[len(PIECES):]):
            if box[2] < HELD_FROM:
                acc = tail_call(meta, a_piece, b_blk, b_rcv, acc, box)
            else:
                out = end_call(a_piece, held, acc, out, row_last, box)
        return out

    spec_in = P("row", "col")
    spec_out = P(("row", "depth"), "col")
    return jax.shard_map(local_mm, mesh=mesh, in_specs=(spec_in, spec_in), out_specs=spec_out, check_vma=False)
```
